32 devices in a mesh: tm: 8 (over z, x), gz: 4 (over y, core).
Axes of the slice: x: 2, y: 2, z: 4, core: 2. Of those that a mesh axis runs over, the one named last changes fastest.
Arguments:
- source: float32 [16, 32, 32, 512], P('tm', None, None, 'gz'), may hold values from -8 to 8
- initial_guess: float32 [16, 32, 32, 512], P('tm', None, None, 'gz'), may hold values from -8 to 8
- diffusivity: float32 [32, 32, 512], P(None, None, 'gz'), may hold values from 0.25 to 2.5
Outputs:
- solution: float32 [16, 32, 32, 512], P('tm', None, None, 'gz')
- residual: float32 [16, 32, 32, 512], P('tm', None, None, 'gz')
The draws below stay inside these ranges and needn't reach their ends.
All inputs are finite; a program needn't handle non-finite values.
Results may differ from the reference program's by a relative error of at most 0.00002.
Values sent between devices are 32-bit elements; how exact they have to be, the bound alone decides.
A program may use at most 128 MiB of HBM per device.

```python
import math
import jax
import jax.numpy as jnp

NX = 32
NY = 32
LEVELS = 5
SWEEPS = 2
CSWEEPS = 4
NT = 16
NZ = 512


def level_of(own_key, extent, pieces, smallest, largest):
    gain = 1.0
    for axis_at, shards_of in pieces:
        steps = jax.random.uniform(jax.random.fold_in(jax.random.fold_in(own_key, 6), axis_at), (shards_of,), jnp.float32, smallest / len(pieces), largest / len(pieces))
        gain = gain * jnp.repeat(jnp.exp(steps), extent[axis_at] // shards_of).reshape((-1,) + (1,) * (len(extent) - 1 - axis_at))
    return gain


def noise(key, extent, spread, reach, pieces=(), dtype=jnp.bfloat16):
    entries = jax.random.normal(key, extent, jnp.float32) * spread
    if len(pieces) > 0:
        entries = level_of(key, extent, pieces, -0.22, 0.18) * entries
    return jnp.clip(entries, min=-reach, max=reach).astype(dtype)


def setup_inputs(seed: int = 0) -> dict:
    streams_of = jax.random.split(jax.random.key(seed), 4)
    source = noise(streams_of[0], (NT, NX, NY, NZ), 1.0, 8.0, ((0, 8), (3, 4)), jnp.float32)
    initial_guess = noise(streams_of[1], (NT, NX, NY, NZ), 1.0, 8.0, ((0, 8), (3, 4)), jnp.float32)
    diffusivity = jnp.clip(jnp.exp(math.log(2.5) - 2.3025851 * jax.random.uniform(streams_of[2], (NX, NY, NZ), jnp.float32) ** level_of(streams_of[2], (NX, NY, NZ), ((2, 4),), -0.2, 0.2)), 0.25, 2.5)
    return dict(source=source, initial_guess=initial_guess, diffusivity=diffusivity)


damping = 0.8
base_coef = 8.0


def operate(values, diffusivity, time_coef):
    before = jnp.concatenate([jnp.zeros_like(values[:1]), values[:-1]], axis=0)
    padded = jnp.pad(values, ((0, 0), (1, 1), (1, 1), (1, 1)))
    beside = padded[:, 2:, 1:-1, 1:-1] + padded[:, :-2, 1:-1, 1:-1]
    beside = beside + padded[:, 1:-1, 2:, 1:-1] + padded[:, 1:-1, :-2, 1:-1]
    beside = beside + padded[:, 1:-1, 1:-1, 2:] + padded[:, 1:-1, 1:-1, :-2]
    return time_coef * (values - before) + diffusivity * (6.0 * values - beside)


def smooth(values, target, diffusivity, time_coef, sweep_count):
    scaled = damping / (time_coef + 6.0 * diffusivity)
    for sweep_num in range(sweep_count):
        values = values + scaled * (target - operate(values, diffusivity, time_coef))
    return values


def cycle(level_num, values, target, diffusivity):
    time_coef = base_coef / (2.0 ** level_num)
    if level_num == LEVELS - 1:
        return smooth(values, target, diffusivity, time_coef, CSWEEPS)
    values = smooth(values, target, diffusivity, time_coef, SWEEPS)
    leftover = target - operate(values, diffusivity, time_coef)
    coarse_res = (leftover[0::2] + leftover[1::2]) * 0.5
    correction = cycle(level_num + 1, jnp.zeros_like(coarse_res), coarse_res, diffusivity)
    values = values + jnp.repeat(correction, 2, axis=0)
    return smooth(values, target, diffusivity, time_coef, SWEEPS)


def reference(source, initial_guess, diffusivity):
    solution = cycle(0, initial_guess, source, diffusivity)
    residual = source - operate(solution, diffusivity, base_coef)
    return solution, residual
```

```python
import jax
import jax.numpy as jnp
from jax import lax
from jax.experimental import pallas as pl
from jax.experimental.pallas import tpu as pltpu
from jax.sharding import PartitionSpec as P

LEVELS = 5
damping = 0.8
base_coef = 8.0
F32 = jnp.float32
MESH = pl.DeviceIdType.MESH
PAD = 8


def make(mesh, nt, nx, ny, nz):
    ntm, ngz = mesh.shape["tm"], mesh.shape["gz"]
    group = 2 ** (LEVELS - 1) // nt
    groups = ntm // group
    half = group // 2
    xb = nx // group
    yp = ny + 2 * PAD
    hi0 = nz // 2
    times = [0] + [group // 2**l for l in range(LEVELS - 1)]
    versions = [0] + [4] * (LEVELS - 2) + [3]
    n_coarse = sum(versions)

    def kernel(src, guess, dif_hbm, sol, res, *scr):
        scr = list(scr)
        V = [scr.pop(0) for _ in range(6)]
        PV = [scr.pop(0) for _ in range(6)]
        f, dif, S0, rb, g1, es, rout = [scr.pop(0) for _ in range(7)]
        A = [None] + [[scr.pop(0) for _ in range(versions[l])] for l in range(1, LEVELS)]
        G = [None] + [scr.pop(0) for _ in range(1, LEVELS)]
        E = [None] + [scr.pop(0) for _ in range(1, LEVELS)]
        S = [S0] + [scr.pop(0) for _ in range(1, LEVELS)]
        ZS, ZL, ZR = [scr.pop(0) for _ in range(3)]
        (load_sem, out_sem, zsend, zlr, zrr, xsend, xlr, xrr, usend, urecv,
         asend, arecv, esend, erecv, psend, precv, tsend, trecv) = scr

        tm, gz = lax.axis_index("tm"), lax.axis_index("gz")
        grp, i = lax.div(tm, group), lax.rem(tm, group)

        def pos_of(k):
            return jnp.where(lax.rem(k, 2) == 0, lax.div(k, 2), group - 1 - lax.div(k, 2))

        def index_of(p):
            return jnp.where(p < half, 2 * p, 2 * (group - 1 - p) + 1)

        p = pos_of(i)
        center = pl.ds(PAD, ny)

        loads = [
            pltpu.make_async_copy(guess, V[0].at[:, pl.ds(1, nx), center, :], load_sem.at[0]),
            pltpu.make_async_copy(src, f, load_sem.at[1]),
            pltpu.make_async_copy(dif_hbm, dif, load_sem.at[2]),
        ]
        for c in loads:
            c.start()

        zpad = jnp.zeros((PAD, nz), F32)
        zrow = jnp.zeros((ny, nz), F32)

        for t in range(nt):
            def clear0(x, _, t=t):
                for v in V:
                    v[t, x, pl.ds(0, PAD), :] = zpad
                    v[t, x, pl.ds(PAD + ny, PAD), :] = zpad
                return 0
            lax.fori_loop(0, nx + 2, clear0, 0)
            for v in V:
                v[t, 0, center, :] = zrow
                v[t, nx + 1, center, :] = zrow
        for l in range(1, LEVELS):
            def clear1(t, _, l=l):
                for a in A[l]:
                    for x in range(xb + 2):
                        a[t, x] = jnp.zeros((yp, nz), F32)
                return 0
            lax.fori_loop(0, times[l] + 1, clear1, 0)

        @pl.when(tm == 0)
        def _():
            def clear2(x, _):
                for v in PV:
                    v[x] = zrow
                return 0
            lax.fori_loop(0, nx, clear2, 0)

        def clear3(n, _):
            ZL[n] = zrow
            ZR[n] = zrow
            return 0
        lax.fori_loop(0, 12 + n_coarse, clear3, 0)

        bar = pltpu.get_barrier_semaphore()

        def greet(where):
            pl.semaphore_signal(bar, inc=1, device_id=where, device_id_type=MESH)

        for j in range(1, group):
            greet({"tm": grp * group + lax.rem(i + j, group)})
        met = group - 1
        for d in (-1, 1):
            there = (gz + d >= 0) & (gz + d < ngz)
            met = met + jnp.where(there, 1, 0)

            @pl.when(there)
            def _(d=d):
                greet({"gz": gz + d})
        if groups > 1:
            for d in (-1, 1):
                there = (grp + d >= 0) & (grp + d < groups)
                met = met + jnp.where(there, group, 0)

                @pl.when(there)
                def _(d=d):
                    for j in range(group):
                        greet({"tm": (grp + d) * group + j})
        pl.semaphore_wait(bar, met)

        def remote(s, d, ss, rs, where):
            return pltpu.make_async_remote_copy(
                src_ref=s, dst_ref=d, send_sem=ss, recv_sem=rs, device_id=where, device_id_type=MESH)

        def step_copy(n, source):
            return remote(source, PV[n], usend.at[n], urecv.at[n], {"tm": tm + 1})

        def step_send(n, source):
            @pl.when(tm < ntm - 1)
            def _():
                step_copy(n, source).start()

        def step_recv(n, source):
            @pl.when(tm > 0)
            def _():
                step_copy(n, source).wait_recv()

        def step_sent(n, source):
            @pl.when(tm < ntm - 1)
            def _():
                step_copy(n, source).wait_send()

        def z_copies(n):
            par = n % 2
            return (remote(ZS.at[n], ZR.at[n], zsend.at[0, par], zrr.at[n], {"gz": gz - 1}),
                    remote(ZS.at[n], ZL.at[n], zsend.at[1, par], zlr.at[n], {"gz": gz + 1}))

        def z_send(n):
            lo, hi = z_copies(n)

            @pl.when(gz > 0)
            def _():
                lo.start()

            @pl.when(gz < ngz - 1)
            def _():
                hi.start()

        def z_wait(n):
            lo, hi = z_copies(n)

            @pl.when(gz > 0)
            def _():
                lo.wait_send()
                hi.wait_recv()

            @pl.when(gz < ngz - 1)
            def _():
                hi.wait_send()
                lo.wait_recv()

        lane = lax.broadcasted_iota(jnp.int32, (ny, nz), 1)

        def pack(acc, val, k):
            acc = jnp.where(lane == k, pltpu.roll(val, k, 1), acc)
            return jnp.where(lane == hi0 + k, pltpu.roll(val, lax.rem(k + hi0 + 1, nz), 1), acc)

        def flux(v, t, x, n, k):
            c = v[t, x, center, :]
            nb = v[t, x + 1, center, :] + v[t, x - 1, center, :]
            nb = nb + v[t, x, pl.ds(PAD + 1, ny), :] + v[t, x, pl.ds(PAD - 1, ny), :]
            left = jnp.where(lane == 0, pltpu.roll(ZL[n], hi0 - k, 1), pltpu.roll(c, 1, 1))
            right = jnp.where(lane == nz - 1, pltpu.roll(ZR[n], nz - 1 - k, 1), pltpu.roll(c, nz - 1, 1))
            return c, 6.0 * c - (nb + right + left)

        def defect(v, t, x, n, k, before, target, d, coef):
            c, lap = flux(v, t, x, n, k)
            return c, target - (coef * (c - before) + d * lap)

        def run(count, fn, n):
            def step(k, acc):
                return pack(acc, fn(k), k)
            ZS[n] = lax.fori_loop(0, count, step, zrow, unroll=2)
            z_send(n)

        def each(count, fn):
            def step(k, _):
                fn(k)
                return 0
            lax.fori_loop(0, count, step, 0, unroll=2)

        def before0(m, pn, t, x):
            return PV[pn][x] if t == 0 else V[m][t - 1, x + 1, center, :]

        def sweep0(m, t):
            n = 2 * m + t

            def fn(x):
                c, r = defect(V[m], t, x + 1, n, x, before0(m, m, t, x), f[t, x], dif[x], base_coef)
                new = c + S0[x] * r
                V[m + 1][t, x + 1, center, :] = new
                return new
            run(nx, fn, n + 2)

        def resid0(m, t, put):
            n = 2 * m + t

            def fn(x):
                _, r = defect(V[m], t, x + 1, n, x, before0(m, m, t, x), f[t, x], dif[x], base_coef)
                put(x, r)
            each(nx, fn)

        last = nt - 1

        def block(m):
            return V[m].at[last, pl.ds(1, nx), center, :]

        step_send(0, guess.at[last])
        for c in loads:
            c.wait()

        for t in (1, 0):
            def first(x, t=t):
                return V[0][t, x + 1, center, :]
            run(nx, first, t)

        def scales(x):
            S0[x] = damping / (base_coef + 6.0 * dif[x])
        each(nx, scales)
        for l in range(1, LEVELS):
            for x in range(xb):
                S[l][x] = damping / (base_coef / 2.0**l + 6.0 * dif[p * xb + x])

        z_wait(1)
        sweep0(0, 1)
        step_send(1, block(1))
        step_recv(0, guess.at[last])
        z_wait(0)
        sweep0(0, 0)
        z_wait(3)
        sweep0(1, 1)
        step_send(2, block(2))
        step_recv(1, block(1))
        z_wait(2)
        sweep0(1, 0)

        def put_rb(x, r):
            rb[x] = r
        z_wait(5)
        resid0(2, 1, put_rb)
        z_wait(4)
        step_recv(2, block(2))

        def put_g(x, r):
            g1[x] = (r + rb[x]) * 0.5
        resid0(2, 0, put_g)
        step_sent(0, guess.at[last])
        step_sent(1, block(1))
        step_sent(2, block(2))

        def a2a(j, to):
            other = lax.rem(i + j, group)
            return remote(g1.at[pl.ds(pos_of(other) * xb, xb)], G[1].at[to], asend.at[j], arecv.at[j],
                          {"tm": grp * group + other})

        for j in range(1, group):
            a2a(j, i).start()
        for x in range(xb):
            G[1][i, x] = g1[p * xb + x]
        for j in range(1, group):
            c = a2a(j, lax.rem(i + group - j, group))
            c.wait_recv()
            c.wait_send()

        slot = [0]

        def halo_copies(l, ver, n):
            a, T = A[l][ver], times[l]
            steps = pl.ds(1, T)
            lo = remote(a.at[steps, 1, center, :], a.at[steps, xb + 1, center, :],
                        xsend.at[0], xrr.at[n], {"tm": grp * group + index_of(lax.max(p - 1, 0))})
            hi = remote(a.at[steps, xb, center, :], a.at[steps, 0, center, :],
                        xsend.at[1], xlr.at[n], {"tm": grp * group + index_of(lax.min(p + 1, group - 1))})
            nxt = None
            if groups > 1:
                nxt = remote(a.at[T, pl.ds(1, xb), center, :], a.at[0, pl.ds(1, xb), center, :],
                             tsend.at[0], trecv.at[n], {"tm": tm + group})
            return lo, hi, nxt

        def fill(l, ver, fn):
            n = slot[0]
            slot[0] += 1
            T = times[l]
            a = A[l][ver]

            def put(k):
                t, x = lax.div(k, xb), lax.rem(k, xb)
                val = fn(t, x, k)
                a[t + 1, x + 1, center, :] = val
                return val
            run(T * xb, put, 12 + n)
            lo, hi, nxt = halo_copies(l, ver, n)

            @pl.when(p > 0)
            def _():
                lo.start()

            @pl.when(p < group - 1)
            def _():
                hi.start()
            if nxt is not None:
                @pl.when(grp < groups - 1)
                def _():
                    nxt.start()
            z_wait(12 + n)

            @pl.when(p > 0)
            def _():
                lo.wait_send()
                hi.wait_recv()

            @pl.when(p < group - 1)
            def _():
                hi.wait_send()
                lo.wait_recv()
            if nxt is not None:
                @pl.when(grp < groups - 1)
                def _():
                    nxt.wait_send()

                @pl.when(grp > 0)
                def _():
                    nxt.wait_recv()
            return 12 + n

        def defect_at(l, ver, n, t, x, k):
            a = A[l][ver]
            return defect(a, t + 1, x + 1, n, k, a[t, x + 1, center, :], G[l][t, x], dif[p * xb + x],
                          base_coef / 2.0**l)

        def relaxed(l, ver, n):
            def fn(t, x, k):
                c, r = defect_at(l, ver, n, t, x, k)
                return c + S[l][x] * r
            return fn

        def finish(l, ver, n):
            fn = relaxed(l, ver, n)

            def put(k):
                t, x = lax.div(k, xb), lax.rem(k, xb)
                E[l][t, x] = fn(t, x, k)
            each(times[l] * xb, put)

        def coarse(l):
            n = fill(l, 0, lambda t, x, k: S[l][x] * G[l][t, x])
            n = fill(l, 1, relaxed(l, 0, n))
            if l == LEVELS - 1:
                n = fill(l, 2, relaxed(l, 1, n))
                finish(l, 2, n)
                return

            def down(k):
                t, x = lax.div(k, xb), lax.rem(k, xb)
                _, ra = defect_at(l, 1, n, 2 * t, x, 2 * t * xb + x)
                _, rc = defect_at(l, 1, n, 2 * t + 1, x, (2 * t + 1) * xb + x)
                G[l + 1][t, x] = (ra + rc) * 0.5
            each(times[l + 1] * xb, down)
            coarse(l + 1)
            n = fill(l, 2, lambda t, x, k: A[l][1][t + 1, x + 1, center, :] + E[l + 1][lax.div(t, 2), x])
            n = fill(l, 3, relaxed(l, 2, n))
            finish(l, 3, n)

        coarse(1)

        ep = PV[5]

        def back(j, at):
            other = lax.rem(i + j, group)
            return remote(E[1].at[other], es.at[pl.ds(at * xb, xb)], esend.at[j], erecv.at[j],
                          {"tm": grp * group + other})

        def ahead(j, at):
            other = lax.rem(i + j, group)
            return other, remote(E[1].at[lax.rem(other + group - 1, group)], ep.at[pl.ds(at * xb, xb)],
                                 psend.at[j], precv.at[j],
                                 {"tm": jnp.where(other == 0, grp + 1, grp) * group + other})

        for j in range(1, group):
            back(j, p).start()
        for j in range(group):
            other, c = ahead(j, p)
            if j > 0:
                @pl.when(other > 0)
                def _(c=c):
                    c.start()
            if groups > 1:
                @pl.when((other == 0) & (grp < groups - 1))
                def _(c=c):
                    c.start()
        for x in range(xb):
            es[p * xb + x] = E[1][i, x]

        @pl.when(i > 0)
        def _():
            for x in range(xb):
                ep[p * xb + x] = E[1][lax.max(i - 1, 0), x]
        for j in range(1, group):
            back(j, pos_of(lax.rem(i + group - j, group))).wait_recv()

        for t in (1, 0):
            def lift(x, t=t):
                val = V[2][t, x + 1, center, :] + es[x]
                V[3][t, x + 1, center, :] = val
                return val
            run(nx, lift, 6 + t)
        z_wait(7)
        sweep0(3, 1)
        step_send(3, block(4))
        for j in range(group):
            _, c = ahead(j, pos_of(lax.rem(i + group - j, group)))
            if j > 0:
                @pl.when(i > 0)
                def _(c=c):
                    c.wait_recv()
            if groups > 1:
                @pl.when((i == 0) & (grp > 0))
                def _(c=c):
                    c.wait_recv()

        def lift_prev(x):
            rb[x] = PV[2][x] + ep[x]
        each(nx, lift_prev)
        z_wait(6)

        def sweep_a(m, prev):
            n = 2 * m

            def fn(x):
                c, r = defect(V[m], 0, x + 1, n, x, prev[x], f[0, x], dif[x], base_coef)
                new = c + S0[x] * r
                V[m + 1][0, x + 1, center, :] = new
                return new
            run(nx, fn, n + 2)

        sweep_a(3, rb)
        z_wait(9)
        sweep0(4, 1)
        step_send(4, block(5))
        outs = [pltpu.make_async_copy(V[5].at[t, pl.ds(1, nx), center, :], sol.at[t], out_sem.at[t])
                for t in range(nt)]
        outs[1].start()
        step_recv(3, block(4))
        z_wait(8)
        sweep_a(4, PV[3])
        outs[0].start()
        z_wait(11)

        def put_r(t):
            def put(x, r):
                rout[t, x] = r
            return put
        resid0(5, 1, put_r(1))
        rcopy = [pltpu.make_async_copy(rout.at[t], res.at[t], out_sem.at[nt + t]) for t in range(nt)]
        rcopy[1].start()
        z_wait(10)
        step_recv(4, block(5))

        def last_res(x):
            _, r = defect(V[5], 0, x + 1, 10, x, PV[4][x], f[0, x], dif[x], base_coef)
            rout[0, x] = r
        each(nx, last_res)
        rcopy[0].start()
        step_sent(3, block(4))
        step_sent(4, block(5))
        for j in range(1, group):
            back(j, p).wait_send()
        for j in range(group):
            other, c = ahead(j, p)
            if j > 0:
                @pl.when(other > 0)
                def _(c=c):
                    c.wait_send()
            if groups > 1:
                @pl.when((other == 0) & (grp < groups - 1))
                def _(c=c):
                    c.wait_send()
        for c in outs + rcopy:
            c.wait()

    full = pltpu.VMEM((nx, ny, nz), F32)
    dma = pltpu.SemaphoreType.DMA
    nzs = 12 + n_coarse
    scratch = [pltpu.VMEM((nt, nx + 2, yp, nz), F32)] * 6 + [full] * 6
    scratch += [pltpu.VMEM((nt, nx, ny, nz), F32), full, full, full, full, full, pltpu.VMEM((nt, nx, ny, nz), F32)]
    for l in range(1, LEVELS):
        scratch += [pltpu.VMEM((times[l] + 1, xb + 2, yp, nz), F32)] * versions[l]
    scratch += [pltpu.VMEM((times[l], xb, ny, nz), F32) for l in range(1, LEVELS)] * 2
    scratch += [pltpu.VMEM((xb, ny, nz), F32)] * (LEVELS - 1)
    scratch += [pltpu.VMEM((nzs, ny, nz), F32)] * 3
    scratch += [dma((3,)), dma((2 * nt,)), dma((2, 2)), dma((nzs,)), dma((nzs,)), dma((2,)), dma((n_coarse,)),
                dma((n_coarse,)), dma((5,)), dma((5,))] + [dma((group,))] * 6 + [dma((1,)), dma((n_coarse,))]
    shape = jax.ShapeDtypeStruct((nt, nx, ny, nz), F32)
    anyspec = pl.BlockSpec(memory_space=pl.ANY)
    return pl.pallas_call(
        kernel,
        out_shape=(shape, shape),
        in_specs=[anyspec] * 3,
        out_specs=(anyspec, anyspec),
        scratch_shapes=scratch,
        compiler_params=pltpu.CompilerParams(collective_id=0, has_side_effects=True, vmem_limit_bytes=56 << 20),
    )


def solution(mesh):
    def body(source, initial_guess, diffusivity):
        return make(mesh, *source.shape)(source, initial_guess, diffusivity)

    placed = (P("tm", None, None, "gz"), P("tm", None, None, "gz"), P(None, None, "gz"))
    return jax.shard_map(
        body,
        mesh=mesh,
        in_specs=placed,
        out_specs=(P("tm", None, None, "gz"), P("tm", None, None, "gz")),
        check_vma=False,
    )
```
